512 devices in a mesh: tm: 16 (over y, x_hi, core), feed: 32 (over x_lo, z).
Axes of the slice: x: 4 (x_hi: 2, x_lo: 2; x = x_hi * 2 + x_lo), y: 4, z: 16, core: 2. Of those that a mesh axis runs over, the one named last changes fastest.
Arguments:
- voltages: bfloat16 [48, 1024, 16384], P('tm', 'feed'), may hold values from -6 to 6
- pfb_taps: float32 [4, 16384], replicated, may hold values from 0.2 to 1
- feed_of_slot: int32 [1024], replicated, may hold values from 0 to 1023, each once
Outputs:
- beam_power: float32 [16, 1024, 8192], P('tm', None, 'feed')
The draws below stay inside these ranges and needn't reach their ends.
Inputs may be any that keep to these rules, and one draw needn't show every extreme that they name: feed_of_slot[256 * r + j] is the feed at position j of cylinder r; every feed stands at exactly one position.
All inputs are finite; a program needn't handle non-finite values.
Results may differ from the reference program's by a relative error of at most 0.0052.
Values may be sent and summed in bfloat16 or wider, within the bound.
A program may use at most 64 MiB of HBM per device.

```python
import math
import jax
import jax.numpy as jnp
from jax import lax

CYLINDERS = 4
COL_FEEDS = 256
SECTION_ONE = 128
SECTION_TWO = 128
FIR_TAPS = 4
SPECTRA_DEV = 3
FEED_COUNT = 1024
BEAM_COUNT = 1024
BLOCK_LEN = 16384
CHANNELS = 8192
SPECTRA = 48
N_TM = 16


def level_of(key, dims, pieces, smallest, top_value):
    level = 1.0
    for axis_at, blocks in pieces:
        steps = jax.random.uniform(jax.random.fold_in(jax.random.fold_in(key, 6), axis_at), (blocks,), jnp.float32, smallest / len(pieces), top_value / len(pieces))
        level = level * jnp.repeat(jnp.exp(steps), dims[axis_at] // blocks).reshape((-1,) + (1,) * (len(dims) - 1 - axis_at))
    return level


def normal_values(key, shape, scale, reach, split=(), kind=jnp.bfloat16):
    factor_of = level_of(key, shape, split, -0.22, 0.18) if split else 1.0
    array = jax.random.normal(key, shape, jnp.float32) * scale * factor_of
    return jnp.minimum(jnp.maximum(array, -reach), reach).astype(kind)


def setup_inputs(seed: int = 0) -> dict:
    key_list = jax.random.split(jax.random.key(seed), 4)
    return {
        "voltages": normal_values(key_list[0], (SPECTRA, FEED_COUNT, BLOCK_LEN), 1.0, 6.0, ((0, 16), (1, 32))),
        "pfb_taps": jnp.clip(jax.random.uniform(key_list[1], (FIR_TAPS, BLOCK_LEN), jnp.float32, 0.2, 1.0), 0.2, 1.0),
        "feed_of_slot": jax.random.permutation(key_list[2], FEED_COUNT).astype(jnp.int32),
    }


def tables(columns, row_count, period, factor):
    row_index = jnp.arange(row_count, dtype=jnp.int32)[:, None]
    col_index = jnp.arange(columns, dtype=jnp.int32)[None, :]
    angles = (row_index * col_index % period).astype(jnp.float32) * (2.0 * math.pi / period)
    return (jnp.cos(angles) * factor, -jnp.sin(angles) * factor)

def rounded(table):
    return table.astype(jnp.bfloat16).astype(jnp.float32)

def channelize(filtered):
    framed = filtered.reshape(FEED_COUNT, SECTION_ONE, SECTION_TWO).astype(jnp.float32)
    one_re, one_im = tables(SECTION_ONE, SECTION_ONE, SECTION_ONE, 1.0)
    one_re, one_im = (rounded(one_re), rounded(one_im))
    hp = lax.Precision.HIGHEST
    first_re = jnp.einsum('kn,fnm->fkm', one_re, framed, precision=hp)
    first_im = jnp.einsum('kn,fnm->fkm', one_im, framed, precision=hp)
    twist_re, twist_im = tables(SECTION_TWO, SECTION_ONE, BLOCK_LEN, 1.0)
    factor = 1.0 / math.sqrt(BLOCK_LEN)
    turned_re = ((first_re * twist_re - first_im * twist_im) * factor).astype(jnp.bfloat16).astype(jnp.float32)
    turned_im = ((first_re * twist_im + first_im * twist_re) * factor).astype(jnp.bfloat16).astype(jnp.float32)
    two_re, two_im = tables(SECTION_TWO, SECTION_TWO // 2, SECTION_TWO, 1.0)
    two_re, two_im = (rounded(two_re), rounded(two_im))
    spec_re = jnp.einsum('qm,fkm->fqk', two_re, turned_re, precision=hp) - jnp.einsum('qm,fkm->fqk', two_im, turned_im, precision=hp)
    spec_im = jnp.einsum('qm,fkm->fqk', two_re, turned_im, precision=hp) + jnp.einsum('qm,fkm->fqk', two_im, turned_re, precision=hp)
    return (spec_re.astype(jnp.bfloat16), spec_im.astype(jnp.bfloat16))

def power_of(spec_re, spec_im, feed_of_slot):
    hp = lax.Precision.HIGHEST
    shape = (CYLINDERS, COL_FEEDS, spec_re.shape[1], spec_re.shape[2])
    grid_re = jnp.take(spec_re, feed_of_slot, axis=0).reshape(shape).astype(jnp.float32)
    grid_im = jnp.take(spec_im, feed_of_slot, axis=0).reshape(shape).astype(jnp.float32)
    col_re, col_im = tables(COL_FEEDS, COL_FEEDS, COL_FEEDS, 1.0 / math.sqrt(COL_FEEDS))
    col_re, col_im = (rounded(col_re), rounded(col_im))
    along_re = jnp.einsum('jf,cfqk->cjqk', col_re, grid_re, precision=hp) - jnp.einsum('jf,cfqk->cjqk', col_im, grid_im, precision=hp)
    along_im = jnp.einsum('jf,cfqk->cjqk', col_re, grid_im, precision=hp) + jnp.einsum('jf,cfqk->cjqk', col_im, grid_re, precision=hp)
    cyl_re, cyl_im = tables(CYLINDERS, CYLINDERS, CYLINDERS, 1.0 / math.sqrt(CYLINDERS))
    beam_re = jnp.einsum('mc,cjqk->mjqk', cyl_re, along_re, precision=hp) - jnp.einsum('mc,cjqk->mjqk', cyl_im, along_im, precision=hp)
    beam_im = jnp.einsum('mc,cjqk->mjqk', cyl_re, along_im, precision=hp) + jnp.einsum('mc,cjqk->mjqk', cyl_im, along_re, precision=hp)
    return (beam_re * beam_re + beam_im * beam_im).reshape(BEAM_COUNT, CHANNELS)

def reference(voltages, pfb_taps, feed_of_slot):

    def one_block(time_block):

        def add_spectrum(position, running):
            spectrum = (time_block * SPECTRA_DEV + position).astype(jnp.int32)
            filtered = jnp.zeros((FEED_COUNT, BLOCK_LEN), jnp.float32)
            for tap_index in range(FIR_TAPS):
                source = (spectrum + tap_index).astype(jnp.int32)
                inside = jnp.where(source < SPECTRA, 1.0, 0.0).astype(jnp.float32)
                clamped = jnp.minimum(source, SPECTRA - 1).astype(jnp.int32)
                voltage_block = lax.dynamic_index_in_dim(voltages, clamped, 0, keepdims=False)
                filtered = filtered + pfb_taps[tap_index][None, :] * (voltage_block.astype(jnp.float32) * inside)
            spec_re, spec_im = channelize(filtered.astype(jnp.bfloat16))
            return running + power_of(spec_re, spec_im, feed_of_slot)
        return lax.fori_loop(0, SPECTRA_DEV, add_spectrum, jnp.zeros((BEAM_COUNT, CHANNELS), jnp.float32))
    return lax.map(one_block, jnp.arange(N_TM, dtype=jnp.int32))
```

```python
import functools
import math

import jax
import jax.numpy as jnp
import numpy as np
from jax import lax
from jax.experimental import pallas as pl
from jax.experimental.pallas import tpu as pltpu
from jax.sharding import PartitionSpec as P

CYLINDERS = 4
COL_FEEDS = 256
ONE = 128
TWO = 128
SPECTRA = 3
FEEDS = 32
PEERS = 32
RING = 16
BLOCK = ONE * TWO
BEAMS = CYLINDERS * COL_FEEDS
CHUNK = 16
CHUNKS = FEEDS // CHUNK
ROWS = 2 * CHUNK
DEPTH = 2 * PEERS * FEEDS
F32 = jnp.float32
BF16 = jnp.bfloat16


def tables(columns, row_count, period, factor):
    index = np.arange(row_count)[:, None] * np.arange(columns)[None, :] % period
    angles = index.astype(np.float32) * np.float32(2.0 * math.pi / period)
    cos = np.cos(angles.astype(np.float64)) * factor
    sin = -np.sin(angles.astype(np.float64)) * factor
    return cos.astype(np.float32), sin.astype(np.float32)


def constants():
    one = np.concatenate(tables(ONE, ONE, ONE, 1.0), axis=0)
    twist = np.stack(tables(TWO, ONE, BLOCK, 1.0 / math.sqrt(BLOCK)))
    two_re, two_im = tables(TWO, TWO // 2, TWO, 1.0)
    upper = np.stack([two_re, -two_im], axis=1)
    lower = np.stack([two_im, two_re], axis=1)
    two = np.stack([upper, lower], axis=1).reshape(TWO, 2 * TWO)
    col = np.concatenate(tables(COL_FEEDS, COL_FEEDS, COL_FEEDS, 1.0 / math.sqrt(COL_FEEDS)), axis=0)
    half = 1.0 / math.sqrt(CYLINDERS)
    return (
        jnp.asarray(one).astype(BF16),
        jnp.asarray(twist),
        jnp.asarray(two).astype(BF16),
        jnp.asarray(col).astype(BF16) * jnp.asarray(half, BF16),
    )


def peer_at(me, dx, dz):
    x_lo, z = me // RING, me % RING
    return ((x_lo + dx) % 2) * RING + (z + dz) % RING


def kernel(
    volts,
    taps_in,
    feeds_in,
    one_in,
    twist_in,
    two_in,
    col_in,
    out,
    held,
    taps,
    feeds,
    one,
    twist,
    two,
    col,
    framed,
    formed,
    sent,
    got,
    beams,
    own_sem,
    table_sem,
    halo_send,
    halo_recv,
    send_sem,
    recv_sem,
    keep_sem,
):
    me = lax.axis_index("feed")
    tm = lax.axis_index("tm")
    tm_count = lax.axis_size("tm")
    earlier = (tm + tm_count - 1) % tm_count
    later = (tm + 1) % tm_count

    own = pltpu.make_async_copy(volts, held.at[pl.ds(0, SPECTRA)], own_sem)
    own.start()
    loads = []
    for index, (src, dst) in enumerate(
        [
            (taps_in, taps),
            (feeds_in, feeds),
            (one_in, one),
            (twist_in, twist),
            (two_in, two),
            (col_in, col),
        ]
    ):
        load = pltpu.make_async_copy(src, dst, table_sem.at[index])
        load.start()
        loads.append(load)

    barrier = pltpu.get_barrier_semaphore()

    def greet(step, carry):
        pl.semaphore_signal(barrier, inc=1, device_id={"feed": (me + step) % PEERS})
        return carry

    pl.semaphore_signal(barrier, inc=1, device_id={"tm": earlier})
    pl.semaphore_signal(barrier, inc=1, device_id={"tm": later})
    lax.fori_loop(1, PEERS, greet, 0)
    pl.semaphore_wait(barrier, PEERS + 1)

    def halo(block, chunk):
        rows = pl.ds(chunk * CHUNK, CHUNK)
        return pltpu.make_async_remote_copy(
            src_ref=volts.at[block, rows],
            dst_ref=held.at[SPECTRA + block, rows],
            send_sem=halo_send.at[block, chunk],
            recv_sem=halo_recv.at[block, chunk],
            device_id={"tm": earlier},
        )

    for block in range(SPECTRA):
        for chunk in range(CHUNKS):
            halo(block, chunk).start()

    own.wait()
    for load in loads:
        load.wait()
    inside = jnp.where(tm == tm_count - 1, 0.0, 1.0).astype(F32)

    def message(spectrum, chunk, peer):
        return pltpu.make_async_remote_copy(
            src_ref=sent.at[spectrum, chunk, pl.ds(2 * peer, 2)],
            dst_ref=got.at[spectrum, :, pl.ds((chunk * PEERS + me) * ROWS, ROWS)],
            send_sem=send_sem.at[spectrum, chunk],
            recv_sem=recv_sem.at[spectrum, chunk],
            device_id={"feed": peer},
        )

    def keep(spectrum, chunk):
        return pltpu.make_async_copy(
            sent.at[spectrum, chunk, pl.ds(2 * me, 2)],
            got.at[spectrum, :, pl.ds((chunk * PEERS + me) * ROWS, ROWS)],
            keep_sem.at[spectrum, chunk],
        )

    def unit(spectrum, chunk):
        rows = pl.ds(pl.multiple_of(chunk * CHUNK, CHUNK), CHUNK)
        halo(spectrum, chunk).wait_recv()

        def filtered(step, carry):
            for inner in range(8):
                section = step * 8 + inner
                lanes = pl.ds(pl.multiple_of(section * TWO, TWO), TWO)
                total = None
                for tap in range(4):
                    weight = taps[tap : tap + 1, lanes]
                    if spectrum + tap >= SPECTRA:
                        weight = weight * inside
                    term = weight * held[spectrum + tap, rows, lanes].astype(F32)
                    total = term if total is None else total + term
                framed[pl.ds(section, CHUNK, stride=ONE), :] = total
            return carry

        lax.fori_loop(0, ONE // 8, filtered, 0)

        def formed_pair(pair, carry):
            start = pl.multiple_of(pair * 2 * ONE, 2 * ONE)
            both = framed[pl.ds(start, 2 * ONE), :].astype(BF16)
            both = jnp.concatenate([both[:ONE], both[ONE:]], axis=1)
            first = jnp.dot(one[...], both, preferred_element_type=F32)
            twist_re, twist_im = twist[0], twist[1]
            turned = []
            for which in range(2):
                cols = slice(which * TWO, (which + 1) * TWO)
                re, im = first[:ONE, cols], first[ONE:, cols]
                turned_re = (re * twist_re - im * twist_im).astype(BF16)
                turned_im = (re * twist_im + im * twist_re).astype(BF16)
                turned.append(jnp.concatenate([turned_re, turned_im], axis=1))
            turned = jnp.concatenate(turned, axis=0)
            spectra = lax.dot_general(
                two[...], turned, (((1,), (1,)), ((), ())), preferred_element_type=F32
            )
            formed[pl.ds(2 * pair, TWO, stride=CHUNK), :] = spectra[:, :ONE]
            formed[pl.ds(2 * pair + 1, TWO, stride=CHUNK), :] = spectra[:, ONE:]
            return carry

        lax.fori_loop(0, CHUNK // 2, formed_pair, 0)

        def packed(step, carry):
            for inner in range(4):
                row = step * 4 + inner
                start = pl.multiple_of(row * ROWS, ROWS)
                sent[spectrum, chunk, row] = formed[pl.ds(start, ROWS), :].astype(BF16)
            return carry

        lax.fori_loop(0, 2 * PEERS // 4, packed, 0)

        message(spectrum, chunk, peer_at(me, 1, 0)).start()

        def spread(step, carry):
            far = RING // 2 - (step + 1) // 2
            dz = jnp.where(step % 2 == 0, far, RING - far)
            message(spectrum, chunk, peer_at(me, 0, dz)).start()
            message(spectrum, chunk, peer_at(me, 1, dz)).start()
            return carry

        lax.fori_loop(0, RING - 1, spread, 0)
        keep(spectrum, chunk).start()

    def units(spectrum):
        def body(chunk, carry):
            unit(spectrum, chunk)
            return carry

        lax.fori_loop(0, CHUNKS, body, 0)

    def build(tile, carry):
        at = lax.broadcasted_iota(jnp.int32, (256, COL_FEEDS), 0) + tile * 256
        chunk, rest = at // (PEERS * ROWS), at % (PEERS * ROWS)
        feed = (rest // ROWS) * FEEDS + chunk * CHUNK + rest % CHUNK
        lane = lax.broadcasted_iota(jnp.int32, (COL_FEEDS, 256), 1)
        real = (lane // CHUNK) % 2 == 0
        upper, lower = [], []
        for r in range(CYLINDERS):
            row = jnp.concatenate([feeds[2 * r : 2 * r + 1], feeds[2 * r + 1 : 2 * r + 2]], axis=1)
            hot = jnp.where(row == feed, 1.0, 0.0).astype(BF16)
            moved = lax.dot_general(
                col[...], hot, (((1,), (1,)), ((), ())), preferred_element_type=F32
            )
            re, im = moved[:COL_FEEDS], moved[COL_FEEDS:]
            upper.append(jnp.where(real, re, -im))
            lower.append(jnp.where(real, im, re))
        cols = pl.ds(pl.multiple_of(tile * 256, 256), 256)
        for m in range(CYLINDERS):
            top = bottom = None
            for r in range(CYLINDERS):
                turn = m * r % 4
                a, c = upper[r], lower[r]
                a, c = [(a, c), (c, -a), (-a, -c), (-c, a)][turn]
                top = a if top is None else top + a
                bottom = c if bottom is None else bottom + c
            beams[0, pl.ds(m * COL_FEEDS, COL_FEEDS), cols] = top.astype(BF16)
            beams[1, pl.ds(m * COL_FEEDS, COL_FEEDS), cols] = bottom.astype(BF16)
        return carry

    def arrived(spectrum):
        for chunk in range(CHUNKS):
            rows = pl.ds(chunk * PEERS * ROWS, (PEERS - 1) * ROWS)
            part = got.at[spectrum, :, rows]
            pltpu.make_async_copy(part, part, recv_sem.at[spectrum, chunk]).wait()
            keep(spectrum, chunk).wait()

    def beam(spectrum):
        arrived(spectrum)

        def body(tile, carry):
            rows = pl.ds(pl.multiple_of(tile * 256, 256), 256)
            right = jnp.concatenate([got[spectrum, 0], got[spectrum, 1]], axis=1)
            re = jnp.dot(beams[0, rows, :], right, preferred_element_type=F32)
            im = jnp.dot(beams[1, rows, :], right, preferred_element_type=F32)
            power = re * re + im * im
            if spectrum == 0:
                out[0, rows, :] = power
            else:
                out[0, rows, :] += power
            return carry

        lax.fori_loop(0, BEAMS // 256, body, 0)

    units(0)
    lax.fori_loop(0, DEPTH // 256, build, 0)
    units(1)
    beam(0)
    units(2)
    beam(1)
    beam(2)

    for block in range(SPECTRA):
        for chunk in range(CHUNKS):
            halo(block, chunk).wait_send()
            part = sent.at[block, chunk, pl.ds(0, 2 * (PEERS - 1))]
            pltpu.make_async_copy(part, part, send_sem.at[block, chunk]).wait()


def on_device(voltages, pfb_taps, feed_of_slot):
    one, twist, two, col = constants()
    anywhere = pl.BlockSpec(memory_space=pl.ANY)
    dma = pltpu.SemaphoreType.DMA
    return pl.pallas_call(
        kernel,
        out_shape=jax.ShapeDtypeStruct((1, BEAMS, 2 * ONE), F32),
        in_specs=[anywhere] * 7,
        out_specs=pl.BlockSpec(memory_space=pltpu.VMEM),
        scratch_shapes=[
            pltpu.VMEM((2 * SPECTRA, FEEDS, BLOCK), BF16),
            pltpu.VMEM((4, BLOCK), F32),
            pltpu.VMEM((8, 128), jnp.int32),
            pltpu.VMEM((2 * ONE, ONE), BF16),
            pltpu.VMEM((2, ONE, TWO), F32),
            pltpu.VMEM((TWO, 2 * TWO), BF16),
            pltpu.VMEM((2 * COL_FEEDS, COL_FEEDS), BF16),
            pltpu.VMEM((CHUNK * ONE, TWO), F32),
            pltpu.VMEM((TWO * CHUNK, ONE), F32),
            pltpu.VMEM((SPECTRA, CHUNKS, 2 * PEERS, ROWS, ONE), BF16),
            pltpu.VMEM((SPECTRA, 2, DEPTH, ONE), BF16),
            pltpu.VMEM((2, BEAMS, DEPTH), BF16),
            dma,
            dma((6,)),
            dma((SPECTRA, CHUNKS)),
            dma((SPECTRA, CHUNKS)),
            dma((SPECTRA, CHUNKS)),
            dma((SPECTRA, CHUNKS)),
            dma((SPECTRA, CHUNKS)),
        ],
        compiler_params=pltpu.CompilerParams(
            collective_id=0, has_side_effects=True, vmem_limit_bytes=52 * 1024 * 1024
        ),
        name="channel_beams",
    )(voltages, pfb_taps, feed_of_slot.reshape(8, 128), one, twist, two, col)


def solution(mesh):
    in_specs = (P("tm", "feed", None), P(), P())
    out_specs = P("tm", None, "feed")
    return jax.shard_map(
        on_device, mesh=mesh, in_specs=in_specs, out_specs=out_specs, check_vma=False
    )
```
